8 devices in a mesh: replica: 2 (over z, y), data: 4 (over x, core).
Axes of the slice: x: 2, y: 2, z: 1, core: 2. Of those that a mesh axis runs over, the one named last changes fastest.
Arguments:
- inp_rows: bfloat16 [8192, 1536], P(('replica', 'data'))
- out_grad: bfloat16 [8192, 1536], P(('replica', 'data'))
- w_up: bfloat16 [2, 1536, 8960], replicated
- w_down: bfloat16 [2, 8960, 1536], replicated
- master_up: float32 [2, 1536, 8960], P(None, 'data')
- master_down: float32 [2, 8960, 1536], P(None, 'data')
- mom_up: float32 [2, 1536, 8960], P(None, 'data')
- mom_down: float32 [2, 8960, 1536], P(None, 'data')
- var_up: float32 [2, 1536, 8960], P(None, 'data')
- var_down: float32 [2, 8960, 1536], P(None, 'data')
- clip_norm: float32 [], replicated
Outputs:
- output 1: bfloat16 [2, 1536, 8960], replicated
- output 2: bfloat16 [2, 8960, 1536], replicated
- output 3: float32 [2, 1536, 8960], P(None, 'data')
- output 4: float32 [2, 8960, 1536], P(None, 'data')
- output 5: float32 [2, 1536, 8960], P(None, 'data')
- output 6: float32 [2, 8960, 1536], P(None, 'data')
- output 7: float32 [2, 1536, 8960], P(None, 'data')
- output 8: float32 [2, 8960, 1536], P(None, 'data')
- output 9: float32 [], replicated
All inputs are finite; a program needn't handle non-finite values.
Results may differ from the reference program's by a relative error of at most 0.00917307.
Values are sent between devices in bfloat16 or wider.
A program may use at most 2.25 GiB of HBM per device.

```python
import jax
import jax.numpy as jnp
from jax import lax

D = 1536
FF = 8960
B_LOCAL = 1024
REPLICA = 2
DATA = 4
STEP = 10
DEVICES = REPLICA * DATA
ROWS = B_LOCAL * DEVICES
BETA1 = 0.9
BETA2 = 0.95
ADAM_EPS = 1e-8
LEARN_RATE = 5e-3
NORM_EPS = 1e-6
BIAS_ONE = 1.0 - BETA1 ** STEP
BIAS_TWO = 1.0 - BETA2 ** STEP


def gelu_value(pre_act):
    return pre_act * (0.5 + 0.5 * lax.erf(pre_act * 0.7071067811865476))


def gelu_slope(pre_act):
    return 0.5 + 0.5 * lax.erf(pre_act * 0.7071067811865476) + pre_act * jnp.exp(-0.5 * pre_act * pre_act) * 0.3989422804014327


def matmul(left_mat, right_mat):
    return jnp.dot(left_mat, right_mat, preferred_element_type=jnp.float32)


def device_grads(inp_rows, out_grad, w_up, w_down):
    pre_one = matmul(inp_rows, w_up[0]).astype(jnp.bfloat16)
    act_one = gelu_value(pre_one.astype(jnp.float32)).astype(jnp.bfloat16)
    mid_rows = matmul(act_one, w_down[0]).astype(jnp.bfloat16)
    pre_two = matmul(mid_rows, w_up[1]).astype(jnp.bfloat16)
    act_two = gelu_value(pre_two.astype(jnp.float32)).astype(jnp.bfloat16)
    grad_down2 = matmul(act_two.T, out_grad)
    dact_two = matmul(out_grad, w_down[1].T).astype(jnp.bfloat16)
    dpre_two = (dact_two.astype(jnp.float32) * gelu_slope(pre_two.astype(jnp.float32))).astype(jnp.bfloat16)
    grad_up2 = matmul(mid_rows.T, dpre_two)
    dmid_rows = matmul(dpre_two, w_up[1].T).astype(jnp.bfloat16)
    grad_down1 = matmul(act_one.T, dmid_rows)
    dact_one = matmul(dmid_rows, w_down[0].T).astype(jnp.bfloat16)
    dpre_one = (dact_one.astype(jnp.float32) * gelu_slope(pre_one.astype(jnp.float32))).astype(jnp.bfloat16)
    grad_up1 = matmul(inp_rows.T, dpre_one)
    return jnp.stack([grad_up1, grad_up2]), jnp.stack([grad_down1, grad_down2])


def mean_grads(inp_rows, out_grad, w_up, w_down):
    inp_blocks = inp_rows.reshape(DEVICES, B_LOCAL, D)
    grad_blocks = out_grad.reshape(DEVICES, B_LOCAL, D)

    def scan_step(carry_sums, block_pair):
        up_part, down_part = device_grads(block_pair[0], block_pair[1], w_up, w_down)
        return (carry_sums[0] + up_part, carry_sums[1] + down_part), None

    zero_carry = (jnp.zeros((2, D, FF), jnp.float32), jnp.zeros((2, FF, D), jnp.float32))
    totals, unused = lax.scan(scan_step, zero_carry, (inp_blocks, grad_blocks))
    return totals[0] / DEVICES, totals[1] / DEVICES


def adam_update(grad_vals, master_vals, mom_vals, var_vals, clip_scale):
    new_mom = BETA1 * mom_vals + (1.0 - BETA1) * clip_scale * grad_vals
    new_var = BETA2 * var_vals + (1.0 - BETA2) * (clip_scale * clip_scale) * (grad_vals * grad_vals)
    new_master = master_vals - LEARN_RATE * (new_mom / BIAS_ONE) / (jnp.sqrt(new_var / BIAS_TWO) + ADAM_EPS)
    return new_master, new_mom, new_var


def setup_inputs(seed: int = 0) -> dict:
    keys = jax.random.split(jax.random.key(seed), 9)
    inp_rows = jax.random.normal(keys[0], (ROWS, D), jnp.float32).astype(jnp.bfloat16)
    out_grad = jax.random.normal(keys[1], (ROWS, D), jnp.float32).astype(jnp.bfloat16)
    down_gain = jnp.array([1.6, 1.4], jnp.float32).reshape(2, 1, 1)
    master_up = jax.random.normal(keys[2], (2, D, FF), jnp.float32) * D ** -0.5
    master_down = jax.random.normal(keys[3], (2, FF, D), jnp.float32) * down_gain * FF ** -0.5
    w_up = master_up.astype(jnp.bfloat16)
    w_down = master_down.astype(jnp.bfloat16)
    grad_up, grad_down = mean_grads(inp_rows, out_grad, w_up, w_down)
    true_norm = jnp.sqrt(jnp.sum(grad_up * grad_up) + jnp.sum(grad_down * grad_down))
    clip_frac = jax.random.uniform(keys[4], (), jnp.float32, minval=0.3, maxval=0.7)
    up_size = clip_frac * jnp.sqrt(jnp.mean(grad_up * grad_up, axis=(1, 2), keepdims=True))
    down_size = clip_frac * jnp.sqrt(jnp.mean(grad_down * grad_down, axis=(1, 2), keepdims=True))
    mom_up = (1.0 - BETA1) * up_size * jax.random.normal(keys[5], (2, D, FF), jnp.float32)
    mom_down = (1.0 - BETA1) * down_size * jax.random.normal(keys[6], (2, FF, D), jnp.float32)
    var_up = (1.0 - BETA2) * up_size * up_size * jax.random.uniform(keys[7], (2, D, FF), jnp.float32, minval=0.25, maxval=2.0)
    var_down = (1.0 - BETA2) * down_size * down_size * jax.random.uniform(keys[8], (2, FF, D), jnp.float32, minval=0.25, maxval=2.0)
    return {'inp_rows': inp_rows, 'out_grad': out_grad, 'w_up': w_up, 'w_down': w_down, 'master_up': master_up, 'master_down': master_down, 'mom_up': mom_up, 'mom_down': mom_down, 'var_up': var_up, 'var_down': var_down, 'clip_norm': clip_frac * true_norm}


def reference(inp_rows, out_grad, w_up, w_down, master_up, master_down, mom_up, mom_down, var_up, var_down, clip_norm):
    grad_up, grad_down = mean_grads(inp_rows, out_grad, w_up, w_down)
    grad_norm = jnp.sqrt(jnp.sum(grad_up * grad_up) + jnp.sum(grad_down * grad_down))
    clip_scale = jnp.minimum(1.0, clip_norm / (grad_norm + NORM_EPS))
    master_up_new, mom_up_new, var_up_new = adam_update(grad_up, master_up, mom_up, var_up, clip_scale)
    master_down_new, mom_down_new, var_down_new = adam_update(grad_down, master_down, mom_down, var_down, clip_scale)
    return (master_up_new.astype(jnp.bfloat16), master_down_new.astype(jnp.bfloat16), master_up_new, master_down_new, mom_up_new, mom_down_new, var_up_new, var_down_new, grad_norm)
```

```python
import jax
import jax.numpy as jnp
from jax import lax
from jax.sharding import PartitionSpec as P


BETA1 = 0.9
BETA2 = 0.95
ADAM_EPS = 1e-8
LEARN_RATE = 5e-3
NORM_EPS = 1e-6
STEP = 10
BIAS_ONE = 1.0 - BETA1 ** STEP
BIAS_TWO = 1.0 - BETA2 ** STEP
F32 = jnp.float32
BF16 = jnp.bfloat16
CHUNKS = {'d2': 2, 'u2': 2, 'd1': 2, 'u1': 4}


def gelu_value(pre_act):
    return pre_act * (0.5 + 0.5 * lax.erf(pre_act * 0.7071067811865476))


def gelu_slope(pre_act):
    return 0.5 + 0.5 * lax.erf(pre_act * 0.7071067811865476) + pre_act * jnp.exp(-0.5 * pre_act * pre_act) * 0.3989422804014327


def mul(left, right, left_dim, right_dim):
    return lax.dot_general(left, right, (((left_dim,), (right_dim,)), ((), ())), preferred_element_type=F32)


def act(pre):
    return gelu_value(pre.astype(F32)).astype(BF16)


def back(dact, pre):
    return (dact.astype(F32) * gelu_slope(pre.astype(F32))).astype(BF16)


def adam_parts(grad_vals, mom_vals, var_vals, clip_scale):
    new_mom = BETA1 * mom_vals + (1.0 - BETA1) * clip_scale * grad_vals
    new_var = BETA2 * var_vals + (1.0 - BETA2) * (clip_scale * clip_scale) * (grad_vals * grad_vals)
    return new_mom, new_var


def adam_master(new_mom, new_var, master_vals):
    return master_vals - LEARN_RATE * (new_mom / BIAS_ONE) / (jnp.sqrt(new_var / BIAS_TWO) + ADAM_EPS)


def solution(mesh):
    replicas, shards = mesh.shape['replica'], mesh.shape['data']
    total_devices = replicas * shards
    batch_spec = P(('replica', 'data'), None)
    whole_spec = P()
    shard_spec = P(None, 'data', None)
    along_x = [(i, i ^ 2) for i in range(shards)]
    along_core = [(i, i ^ 1) for i in range(shards)]
    along_y = [(i, i ^ 1) for i in range(replicas)]

    def swap_x(val):
        return lax.ppermute(val, 'data', along_x)

    def swap_c(val):
        return lax.ppermute(val, 'data', along_core)

    def swap_y(val):
        return lax.ppermute(val, 'replica', along_y)

    def device_step(inp_rows, out_grad, w_up, w_down, master_up, master_down, mom_up, mom_down, var_up, var_down, clip_norm):
        rep = lax.axis_index('replica')
        dat = lax.axis_index('data')
        own_x, own_c = dat // 2, dat % 2
        dim, hid = w_up.shape[1], w_up.shape[2]
        up_rows, down_rows = dim // shards, hid // shards
        half_dim, half_hid = dim // 2, hid // 2

        inp_far = swap_y(inp_rows)
        grad_far = swap_y(out_grad)
        up_one, up_two = w_up[0], w_up[1]
        down_one, down_two = w_down[0], w_down[1]

        pre_near = mul(up_one, inp_rows, 0, 1).astype(BF16)
        act_near = lax.optimization_barrier(act(pre_near))
        mid_near = mul(act_near, down_one, 0, 0).astype(BF16)
        pre_far = mul(up_one, inp_far, 0, 1).astype(BF16)
        act_far = lax.optimization_barrier(act(pre_far))
        mid_far = mul(act_far, down_one, 0, 0).astype(BF16)
        mid_all = jnp.concatenate([mid_near, mid_far], axis=0)
        pre_two = mul(up_two, mid_all, 0, 1).astype(BF16)
        act_two = act(pre_two)
        dy_all = jnp.concatenate([out_grad, grad_far], axis=0)

        pieces = {}

        def reduce_piece(make, name, axis, size):
            far_x, far_c = 1 - own_x, 1 - own_c
            unit = 128 if axis else 16
            count = CHUNKS[name]
            ends = [unit * ((size // unit * (idx + 1) + count - 1) // count) for idx in range(count)]
            spans = list(zip([0] + ends[:-1], [end - start for start, end in zip([0] + ends[:-1], ends)]))

            def summed(x_idx):
                sent = []
                for span in spans:
                    part = make(x_idx, far_c, *span)
                    sent.append(swap_c(part))
                sums = []
                for idx, span in enumerate(spans):
                    sums.append(make(x_idx, own_c, *span) + sent[idx])
                return sums

            sum_far = summed(far_x)
            from_x = []
            for val in sum_far:
                from_x.append(swap_x(val))
            sum_own = summed(own_x)
            near_parts, far_parts, squares = [], [], 0.0
            for idx, val in enumerate(sum_own):
                came = from_x[idx]
                if near_parts:
                    came, near_parts[-1] = lax.optimization_barrier((came, near_parts[-1]))
                grad = (val + came) / total_devices
                squares = squares + jnp.sum(grad * grad)
                near_parts.append(grad)
                far_parts.append(swap_y(grad))
            pieces[name] = (jnp.concatenate(near_parts, axis=axis), squares, near_parts, far_parts, spans, axis)

        def down_maker(acts, grads):
            def make(x_idx, c_idx, start, size):
                total = None
                for act_t, grad in zip(acts, grads):
                    lhs = lax.dynamic_slice(act_t, ((2 * x_idx + c_idx) * down_rows + start, 0), (size, act_t.shape[1]))
                    rhs = lax.dynamic_slice(grad, (0, rep * half_dim), (grad.shape[0], half_dim))
                    part = mul(lhs, rhs, 1, 0)
                    total = part if total is None else total + part
                return total

            return make

        def up_maker(inps, dpres):
            def make(x_idx, c_idx, start, size):
                total = None
                for inp, dpre in zip(inps, dpres):
                    lhs = lax.dynamic_slice(inp, (0, (2 * x_idx + c_idx) * up_rows), (inp.shape[0], up_rows))
                    rhs = lax.dynamic_slice(dpre, (rep * half_hid + start, 0), (size, dpre.shape[1]))
                    part = mul(lhs, rhs, 0, 1)
                    total = part if total is None else total + part
                return total

            return make

        reduce_piece(down_maker([act_two], [dy_all]), 'd2', 0, down_rows)
        dact_two = mul(down_two, dy_all, 1, 1).astype(BF16)
        dpre_two = back(dact_two, pre_two)
        reduce_piece(up_maker([mid_all], [dpre_two]), 'u2', 1, half_hid)
        dmid = mul(dpre_two, up_two, 0, 1).astype(BF16)
        dmid_near, dmid_far = lax.optimization_barrier((dmid[:inp_rows.shape[0]], dmid[inp_rows.shape[0]:]))
        reduce_piece(down_maker([act_near, act_far], [dmid_near, dmid_far]), 'd1', 0, down_rows)
        dpre_near = back(mul(down_one, dmid_near, 1, 1).astype(BF16), pre_near)
        dpre_far = back(mul(down_one, dmid_far, 1, 1).astype(BF16), pre_far)
        reduce_piece(up_maker([inp_rows, inp_far], [dpre_near, dpre_far]), 'u1', 1, half_hid)

        local_sq = sum(pieces[name][1] for name in ('d2', 'u2', 'd1', 'u1'))
        grad_norm = jnp.sqrt(lax.psum(local_sq, ('replica', 'data')))
        clip_scale = jnp.minimum(1.0, clip_norm / (grad_norm + NORM_EPS))

        states = {'d1': (master_down, mom_down, var_down, 0), 'd2': (master_down, mom_down, var_down, 1),
                  'u1': (master_up, mom_up, var_up, 0), 'u2': (master_up, mom_up, var_up, 1)}
        order = ('d2', 'u2', 'd1', 'u1')
        gathered = {}
        scale = clip_scale
        for name in order:
            master, mom, var, layer = states[name]
            near = pieces[name][0]
            cols = near.shape[1]
            cut = [lax.dynamic_slice(arr, (layer, 0, rep * cols), (1, near.shape[0], cols))[0] for arr in (master, mom, var)]
            mom_new, var_new = adam_parts(near, cut[1], cut[2], scale)
            half_new = adam_master(mom_new, var_new, cut[0]).astype(BF16)
            half_new, scale = lax.optimization_barrier((half_new, scale))
            from_x = swap_x(half_new)
            from_xy = swap_y(from_x)
            from_xc = swap_c(from_x)
            from_xyc = swap_c(from_xy)
            gathered[name] = (from_x, from_xc, from_xy, from_xyc)

        near_all, far_all = {}, {}
        for names in (('d1', 'd2'), ('u1', 'u2')):
            group = lax.optimization_barrier(([pieces[name][2:4] for name in names], scale))[0]
            for name, (near, far) in zip(names, group):
                near_all[name], far_all[name] = near, far

        def laid_grad(names, shape):
            grad = jnp.zeros(shape, F32)
            for layer, name in enumerate(names):
                spans, axis = pieces[name][4:]
                cols = shape[2] // 2
                for parts, side in ((near_all[name], rep), (far_all[name], 1 - rep)):
                    for part, span in zip(parts, spans):
                        start = (layer, 0, side * cols + span[0]) if axis else (layer, span[0], side * cols)
                        grad = lax.dynamic_update_slice(grad, part[None], start)
            return grad

        def full_update(grad, master, mom, var):
            mom_new, var_new = adam_parts(grad, mom, var, scale)
            master_new = adam_master(mom_new, var_new, master)
            return master_new, mom_new, var_new, master_new.astype(BF16)

        def assemble(names, shard, shape):
            rows = shard.shape[1]
            other = swap_c(shard)
            out = jnp.zeros(shape, BF16)
            out = lax.dynamic_update_slice(out, shard, (0, (2 * own_x + own_c) * rows, 0))
            out = lax.dynamic_update_slice(out, other, (0, (2 * own_x + 1 - own_c) * rows, 0))
            far_x = 2 * (1 - own_x)
            for name in order:
                if name not in names:
                    continue
                layer = states[name][3]
                from_x, from_xc, from_xy, from_xyc = gathered[name]
                cols = from_x.shape[1]
                out = lax.dynamic_update_slice(out, from_x[None], (layer, (far_x + own_c) * rows, rep * cols))
                out = lax.dynamic_update_slice(out, from_xc[None], (layer, (far_x + 1 - own_c) * rows, rep * cols))
                out = lax.dynamic_update_slice(out, from_xy[None], (layer, (far_x + own_c) * rows, (1 - rep) * cols))
                out = lax.dynamic_update_slice(out, from_xyc[None], (layer, (far_x + 1 - own_c) * rows, (1 - rep) * cols))
            return out

        grad_down = laid_grad(('d1', 'd2'), master_down.shape)
        grad_up = laid_grad(('u1', 'u2'), master_up.shape)
        master_down_new, mom_down_new, var_down_new, shard_down = lax.optimization_barrier(full_update(grad_down, master_down, mom_down, var_down))
        master_up_new, mom_up_new, var_up_new, shard_up = lax.optimization_barrier(full_update(grad_up, master_up, mom_up, var_up))
        w_down_new = assemble(('d1', 'd2'), shard_down, w_down.shape)
        w_up_new = assemble(('u1', 'u2'), shard_up, w_up.shape)
        return (w_up_new, w_down_new, master_up_new, master_down_new, mom_up_new, mom_down_new, var_up_new, var_down_new, grad_norm)


    return jax.shard_map(device_step, mesh=mesh, in_specs=(batch_spec, batch_spec, whole_spec, whole_spec, shard_spec, shard_spec, shard_spec, shard_spec, shard_spec, shard_spec, whole_spec), out_specs=(whole_spec, whole_spec, shard_spec, shard_spec, shard_spec, shard_spec, shard_spec, shard_spec, whole_spec), check_vma=False)
```
